32 devices in a mesh: dp: 8 (over z, x), feat: 4 (over y, core).
Axes of the slice: x: 2, y: 2, z: 4, core: 2. Of those that a mesh axis runs over, the one named last changes fastest.
Arguments:
- embeddings: bfloat16 [32768, 2048], P('dp', 'feat'), may hold values from -6 to 6
- sample_owner: int32 [32768], P('dp'), may hold values from 0 to 191
- lloyd_assign: int32 [2, 192], P(None, 'dp'), may hold values from 0 to 127
- init_centroids: float32 [128, 2048], P('dp', 'feat'), may hold values from -6 to 6
Outputs:
- centroids: float32 [128, 2048], P('dp', 'feat')
- spread: float32 [2, 192], P(None, 'dp')
The draws below stay inside these ranges and needn't reach their ends.
All inputs are finite; a program needn't handle non-finite values.
Results may differ from the reference program's by a relative error of at most 0.0003.
Values sent between devices are 32-bit elements; how exact they have to be, the bound alone decides.
No kernel may reach another device: no remote copies, remote signals or barrier semaphores. Data moves between devices by JAX's collectives and lax.ppermute only.
A program may use at most 64 MiB of HBM per device.

```python
import math
import jax
import jax.numpy as jnp
import numpy as np
from jax import lax

D = 2048
SAMPLES = 32768
C = 192
K = 128


def plant(array, own_key, least, high):
    longest = array.shape.index(max(array.shape))
    spots = []
    for shift in (0, 1):
        where = [jax.random.randint(jax.random.fold_in(own_key, axis), (), 0, length) for axis, length in enumerate(array.shape)]
        where[longest] = (where[longest] + shift) % array.shape[longest]
        spots.append(tuple(where))
    return array.at[spots[0]].set(least).at[spots[1]].set(high)


def shard_levels(own_key, shape, shards, least, high):
    level, own = 1.0, jax.random.fold_in(own_key, 6)
    for position, blocks in shards:
        draws = jnp.exp(jax.random.uniform(jax.random.fold_in(own, position), (blocks,), jnp.float32, least / len(shards), high / len(shards)))
        level = level * jnp.repeat(draws, shape[position] // blocks).reshape([-1 if axis == position else 1 for axis in range(len(shape))])
    return level


def rank_table(number_of, lean):
    loads = [(1 << 20) // math.isqrt(grade ** lean) + 1 for grade in range(1, number_of + 1)]
    scale = 1 + sum(loads) // (1 << 30)
    return np.cumsum(np.array([max(1, weight // scale) for weight in loads]))


def ranked_ids(key, shape, count, skew):
    listing = rank_table(count, skew)
    ticket = jax.random.randint(jax.random.fold_in(key, 1), shape, 0, int(listing[count - 1]))
    grade = jnp.searchsorted(jnp.asarray(listing, jnp.int32), ticket, side="right")
    return jax.random.permutation(jax.random.fold_in(key, 2), count)[grade].astype(jnp.int32)


def noise(stream_key, shape, scale, bound, pieces=(), kind=jnp.bfloat16):
    drawn = jax.random.normal(stream_key, shape, jnp.float32) * scale
    if len(pieces) > 0:
        drawn = shard_levels(stream_key, shape, pieces, -0.22, 0.18) * drawn
    return jnp.clip(drawn, min=-bound, max=bound).astype(kind)


def setup_inputs(seed: int = 0) -> dict:
    keys = jax.random.split(jax.random.key(seed), 5)
    embeddings = noise(keys[0], (SAMPLES, D), 1.0, 6.0, ((0, 8), (1, 4)))
    sample_owner = plant(ranked_ids(keys[1], (SAMPLES,), C, 2), jax.random.fold_in(keys[1], 3), 0, C - 1).astype(jnp.int32)
    lloyd_assign = plant(ranked_ids(keys[2], (2, C), K, 2), jax.random.fold_in(keys[2], 3), 0, K - 1).astype(jnp.int32)
    init_centroids = noise(keys[3], (K, D), 1.0, 6.0, ((0, 8), (1, 4)), jnp.float32)
    return {"embeddings": embeddings, "sample_owner": sample_owner, "lloyd_assign": lloyd_assign, "init_centroids": init_centroids}


EPS = 1e-06

def normalize(rows):
    return rows * lax.rsqrt(lax.optimization_barrier(jnp.mean(rows * rows, axis=1, keepdims=True)) + EPS)

def reference(embeddings, sample_owner, lloyd_assign, init_centroids):
    sums = jax.ops.segment_sum(embeddings.astype(jnp.float32), sample_owner, C)
    counts = jax.ops.segment_sum(jnp.ones(sample_owner.shape, jnp.float32), sample_owner, C)
    means = normalize(sums)
    weighted = counts[:, None] * means
    prev = init_centroids
    spreads = []
    for step in range(2):
        assign = lloyd_assign[step]
        total = jax.ops.segment_sum(weighted, assign, K)
        weight = jax.ops.segment_sum(counts, assign, K)
        fresh = normalize(total)
        current = jnp.where(weight[:, None] > 0, fresh, prev)
        diff = means - jnp.take(fresh, assign, axis=0)
        spreads.append(lax.optimization_barrier(jnp.mean(diff * diff, axis=1)))
        prev = current
    return (prev, jnp.stack(spreads))
```

```python
import functools
import math

import jax
import jax.numpy as jnp
from jax import lax
from jax.experimental import pallas as pl
from jax.experimental.pallas import tpu as pltpu
from jax.sharding import PartitionSpec as P

EPS = 1e-06
LANES = 128
SUBLANES = 8
COUNT_ROW, SQUARE_ROW, LABEL_ROW = 0, 1, 2
HIGHEST = lax.Precision.HIGHEST
F32 = jnp.float32
VMEM = pl.BlockSpec(memory_space=pltpu.VMEM)


def room(*arrays):
    held = sum(4 * math.prod(shape) for shape in arrays)
    return pltpu.CompilerParams(vmem_limit_bytes=min((8 << 20) + 2 * held, 60 << 20))


def swap(x, axis, size, k):
    return lax.ppermute(x, axis, [(i, i ^ k) for i in range(size)])


def sum_over(x, axis):
    size = lax.axis_size(axis)
    if size & (size - 1):
        return lax.psum(x, axis)
    k = 1
    while k < size:
        x = x + swap(x, axis, size, k)
        k *= 2
    return x


def lanes_of(columns):
    ones = jnp.ones((SUBLANES, columns.shape[1]), F32)
    return lax.dot_general(
        ones, columns, (((1,), (1,)), ((), ())), precision=HIGHEST, preferred_element_type=F32
    )


def column_of(row, n):
    r = lax.broadcasted_iota(jnp.int32, (n, row.shape[1]), 0)
    c = lax.broadcasted_iota(jnp.int32, (n, row.shape[1]), 1)
    return jnp.sum(jnp.where(r == c, row, 0.0), axis=1, keepdims=True)


def row_of(column):
    n = column.shape[0]
    r = lax.broadcasted_iota(jnp.int32, (n, LANES), 0)
    c = lax.broadcasted_iota(jnp.int32, (n, LANES), 1)
    return jnp.sum(jnp.where(r == c, column, 0.0), axis=0, keepdims=True)


def sums_kernel(chunk, c_local, relative, owner_ref, emb_ref, *rest):
    outs, (emb, acc, cnt, sems) = rest[:-4], rest[-4:]
    n, feats = emb.shape
    cands = acc.shape[0]
    steps = n // chunk

    def copy(s):
        rows = pl.ds(s * chunk, chunk)
        return pltpu.make_async_copy(emb_ref.at[rows], emb.at[rows], sems.at[s])

    for s in range(steps):
        copy(s).start()
    labels = lax.broadcasted_iota(jnp.int32, (cands, chunk), 0)
    for s in range(steps):
        hit = jnp.where(labels == owner_ref[:, s * chunk : (s + 1) * chunk], 1.0, 0.0)
        fold = hit[:, :LANES]
        for j in range(1, chunk // LANES):
            fold = fold + hit[:, j * LANES : (j + 1) * LANES]
        copy(s).wait()
        part = jnp.dot(
            hit.astype(jnp.bfloat16),
            emb[s * chunk : (s + 1) * chunk, :],
            preferred_element_type=F32,
        )
        if s == 0:
            acc[...] = part
            cnt[...] = fold
        else:
            acc[...] += part
            cnt[...] += fold
    me = lax.axis_index("dp")
    groups = c_local // SUBLANES
    parts = cands // c_local
    for k in range(parts):
        base = (me ^ k if relative else k) * c_local
        dst = outs[k] if relative else outs[0].at[k]
        for q in range(feats // LANES):
            for r in range(groups):
                dst[q * groups + r] = acc[
                    pl.ds(pl.multiple_of(base + r * SUBLANES, SUBLANES), SUBLANES),
                    q * LANES : (q + 1) * LANES,
                ]
        counts = lanes_of(cnt[pl.ds(pl.multiple_of(base, SUBLANES), c_local), :])
        rows = lax.broadcasted_iota(jnp.int32, counts.shape, 0)
        tile = dst.shape[0] - 1
        dst[tile] = jnp.zeros((SUBLANES, LANES), F32)
        dst[tile, :, :c_local] = jnp.where(rows == COUNT_ROW, counts, 0.0)


def partial_sums(embeddings, owner, parts, c_local, relative):
    n, feats = embeddings.shape
    chunk = min(512, n)
    tiles = (c_local // SUBLANES) * (feats // LANES) + 1
    block = (tiles, SUBLANES, LANES)
    if relative:
        out = [jax.ShapeDtypeStruct(block, F32)] * parts
    else:
        out = [jax.ShapeDtypeStruct((parts, *block), F32)]
    return pl.pallas_call(
        functools.partial(sums_kernel, chunk, c_local, relative),
        out_shape=out,
        in_specs=[VMEM, pl.BlockSpec(memory_space=pltpu.HBM)],
        out_specs=[VMEM] * len(out),
        scratch_shapes=[
            pltpu.VMEM((n, feats), embeddings.dtype),
            pltpu.VMEM((parts * c_local, feats), F32),
            pltpu.VMEM((parts * c_local, LANES), F32),
            pltpu.SemaphoreType.DMA((n // chunk,)),
        ],
        compiler_params=pltpu.CompilerParams(vmem_limit_bytes=61 << 20),
        name="candidate_sums",
    )(owner.reshape(1, n), embeddings)


def square_kernel(c_local, assign_ref, *refs):
    blocks, out_ref, sq_ref = refs[:-2], refs[-2], refs[-1]
    tiles = out_ref.shape[0] - 1
    groups = c_local // SUBLANES
    squares = []
    for r in range(groups):
        total = None
        for q in range(tiles // groups):
            t = q * groups + r
            x = blocks[0][t]
            for block in blocks[1:]:
                x = x + block[t]
            out_ref[t] = x
            total = x * x if total is None else total + x * x
        squares.append(total)
    aux = blocks[0][tiles]
    for block in blocks[1:]:
        aux = aux + block[tiles]
    out_ref[tiles] = aux
    steps = assign_ref.shape[0]
    out_ref[tiles, LABEL_ROW : LABEL_ROW + steps, :c_local] = assign_ref[...].astype(F32)
    lanes = lanes_of(jnp.concatenate(squares, axis=0))
    rows = lax.broadcasted_iota(jnp.int32, lanes.shape, 0)
    sq_ref[...] = jnp.zeros_like(sq_ref)
    sq_ref[:, :c_local] = jnp.where(rows == SQUARE_ROW, lanes, 0.0)


def add_and_square(blocks, assign, c_local):
    shape = blocks[0].shape
    return pl.pallas_call(
        functools.partial(square_kernel, c_local),
        out_shape=[jax.ShapeDtypeStruct(shape, F32), jax.ShapeDtypeStruct(shape[1:], F32)],
        in_specs=[VMEM] * (1 + len(blocks)),
        out_specs=[VMEM] * 2,
        compiler_params=room(*[block.shape for block in blocks]),
        name="add_and_square",
    )(assign, *blocks)


def totals_kernel(c_local, k_local, width, slot, own_ref, *refs):
    n_in = len(refs) - 4
    ins, (tot_ref, wgt_ref, q_ref, raw) = refs[:n_in], refs[n_in:]
    tiles = own_ref.shape[0] - 1
    groups = c_local // SUBLANES
    cols = tiles // groups
    steps = tot_ref.shape[0]
    views = []
    for ref in ins:
        views += [ref] if len(ref.shape) == 3 else [ref.at[j] for j in range(ref.shape[0])]
    per = LANES // slot
    aux = []
    for n, view in enumerate(views):
        for r in range(groups):
            at = n * slot + r * SUBLANES
            for q in range(cols):
                raw[at : at + SUBLANES, q * LANES : (q + 1) * LANES] = view[q * groups + r]
        if slot > c_local:
            raw[n * slot + c_local : (n + 1) * slot, :] = jnp.zeros(
                (slot - c_local, cols * LANES), F32
            )
        tile = view[tiles]
        if n % per == 0:
            aux.append(tile)
        else:
            aux[-1] = aux[-1] + pltpu.roll(tile, slot * (n % per), 1)
    aux = jnp.concatenate(aux, axis=1)
    lanes = aux.shape[1]
    if raw.shape[0] > len(views) * slot:
        raw[len(views) * slot :, :] = jnp.zeros((raw.shape[0] - len(views) * slot, cols * LANES), F32)
    count = aux[COUNT_ROW : COUNT_ROW + 1]
    scale = lax.rsqrt(aux[SQUARE_ROW : SQUARE_ROW + 1] / width + EPS)
    own_aux = own_ref[tiles]
    own_scale = lax.rsqrt(column_of(own_aux[SQUARE_ROW : SQUARE_ROW + 1], c_local) / width + EPS)
    first = lax.axis_index("dp") * k_local
    ids = (lax.broadcasted_iota(jnp.int32, (k_local, 1), 0) + first).astype(F32)
    picks, weights = [], []
    for t in range(steps):
        label = LABEL_ROW + t
        own = column_of(own_aux[label : label + 1], c_local)
        keys = jnp.concatenate([ids, own], axis=0)
        match = keys == aux[label : label + 1]
        picks.append(jnp.where(match, count * scale, 0.0))
        weights.append(jnp.sum(jnp.where(match, count, 0.0), axis=1, keepdims=True))
    total = jnp.dot(
        jnp.concatenate(picks, axis=0), raw[...], precision=HIGHEST, preferred_element_type=F32
    )
    means = jnp.concatenate(
        [
            jnp.concatenate([own_ref[q * groups + r] for q in range(cols)], axis=1)
            for r in range(groups)
        ],
        axis=0,
    ) * own_scale
    span = k_local + c_local
    lane = lax.broadcasted_iota(jnp.int32, (c_local, LANES), 1)
    lane_k = lax.broadcasted_iota(jnp.int32, (k_local, LANES), 1)
    q_c = jnp.zeros((c_local, LANES), F32)
    q_k = jnp.zeros((k_local, LANES), F32)
    w_c = jnp.zeros((c_local, LANES), F32)
    w_k = jnp.zeros((k_local, LANES), F32)
    for t in range(steps):
        t_k = total[t * span : t * span + k_local]
        t_c = total[t * span + k_local : (t + 1) * span]
        weight = weights[t]
        near = weight[k_local:]
        center = t_c / jnp.where(near > 0, near, 1.0)
        diff = means - center
        for j, (a, b) in enumerate(((diff, diff), (diff, center), (center, center))):
            q_c = jnp.where(lane == 4 * t + j, jnp.sum(a * b, axis=1, keepdims=True), q_c)
        q_k = jnp.where(lane_k == t, jnp.sum(t_k * t_k, axis=1, keepdims=True), q_k)
        w_c = jnp.where(lane == t, near, w_c)
        w_k = jnp.where(lane_k == t, weight[:k_local], w_k)
        tot_ref[t] = t_k
    q_ref[:c_local] = q_c
    q_ref[c_local:] = q_k
    wgt_ref[:c_local] = w_c
    wgt_ref[c_local:] = w_k


def totals(own, ins, steps, parts, c_local, k_local, feats, width):
    slot = 8
    while slot < c_local:
        slot *= 2
    lanes = -(-parts * slot // LANES) * LANES
    rows = c_local + k_local
    return pl.pallas_call(
        functools.partial(totals_kernel, c_local, k_local, width, slot),
        out_shape=[
            jax.ShapeDtypeStruct((steps, k_local, feats), F32),
            jax.ShapeDtypeStruct((rows, LANES), F32),
            jax.ShapeDtypeStruct((rows, LANES), F32),
        ],
        in_specs=[VMEM] * (1 + len(ins)),
        out_specs=[VMEM] * 3,
        scratch_shapes=[pltpu.VMEM((lanes, feats), F32)],
        compiler_params=room((lanes, 2 * feats)),
        name="cluster_totals",
    )(own, *ins)


def finish_kernel(c_local, width, tot_ref, wgt_ref, q_ref, init_ref, cen_ref, spread_ref):
    steps = tot_ref.shape[0]
    current = init_ref[...]
    for t in range(steps):
        length = q_ref[c_local:, t : t + 1]
        fresh = tot_ref[t] * lax.rsqrt(length / width + EPS)
        current = jnp.where(wgt_ref[c_local:, t : t + 1] > 0, fresh, current)
        near = wgt_ref[:c_local, t : t + 1]
        dd, da, aa = (q_ref[:c_local, 4 * t + j : 4 * t + j + 1] for j in range(3))
        gap = 1.0 - near * lax.rsqrt(near * near * (aa / width) + EPS)
        spread = (dd + gap * (2.0 * da + gap * aa)) / width
        spread_ref[t : t + 1, :] = row_of(spread)[:, :c_local]
    cen_ref[...] = current


def finish(tot, wgt, q, init, c_local, width):
    return pl.pallas_call(
        functools.partial(finish_kernel, c_local, width),
        out_shape=[
            jax.ShapeDtypeStruct(init.shape, F32),
            jax.ShapeDtypeStruct((tot.shape[0], c_local), F32),
        ],
        in_specs=[VMEM] * 4,
        out_specs=[VMEM] * 2,
        compiler_params=room(tot.shape, init.shape),
        name="finish",
    )(tot, wgt, q, init)


def per_device(embeddings, sample_owner, lloyd_assign, init_centroids):
    parts = lax.axis_size("dp")
    steps, c_local = lloyd_assign.shape
    k_local, feats = init_centroids.shape
    width = feats * lax.axis_size("feat")
    direct = parts <= 16 and parts & (parts - 1) == 0
    blocks = partial_sums(embeddings, sample_owner, parts, c_local, direct)
    if direct:
        blocks = [blocks[0]] + [swap(blocks[k], "dp", parts, k) for k in range(1, parts)]
    else:
        blocks = [lax.psum_scatter(blocks[0], "dp", scatter_dimension=0)]
    own, squares = add_and_square(blocks, lloyd_assign, c_local)
    own = own.at[-1].add(sum_over(squares, "feat"))
    if direct:
        everyone = [own] + [swap(own, "dp", parts, k) for k in range(1, parts)]
    else:
        everyone = [lax.all_gather(own, "dp")]
    tot, wgt, q = totals(own, everyone, steps, parts, c_local, k_local, feats, width)
    q = sum_over(q, "feat")
    centroids, spread = finish(tot, wgt, q, init_centroids, c_local, width)
    return centroids, spread


def solution(mesh):
    in_specs = (P("dp", "feat"), P("dp"), P(None, "dp"), P("dp", "feat"))
    out_specs = (P("dp", "feat"), P(None, "dp"))
    return jax.shard_map(
        per_device, mesh=mesh, in_specs=in_specs, out_specs=out_specs, check_vma=False
    )
```

```python
import functools
import math

import jax
import jax.numpy as jnp
from jax import lax
from jax.experimental import pallas as pl
from jax.experimental.pallas import tpu as pltpu
from jax.sharding import PartitionSpec as P

EPS = 1e-06
LANES = 128
SUBLANES = 8
COUNT_ROW, SQUARE_ROW, LABEL_ROW = 0, 1, 2
HIGHEST = lax.Precision.HIGHEST
F32 = jnp.float32
VMEM = pl.BlockSpec(memory_space=pltpu.VMEM)


def room(*arrays):
    held = sum(4 * math.prod(shape) for shape in arrays)
    return pltpu.CompilerParams(vmem_limit_bytes=min((8 << 20) + 2 * held, 60 << 20))


def swap(x, axis, size, k):
    return lax.ppermute(x, axis, [(i, i ^ k) for i in range(size)])


def sum_over(x, axis):
    size = lax.axis_size(axis)
    if size & (size - 1) or size > 4:
        return lax.psum(x, axis)
    parts = [swap(x, axis, size, k) for k in range(1, size)]
    return functools.reduce(jnp.add, parts, x)


def lanes_of(columns):
    ones = jnp.ones((SUBLANES, columns.shape[1]), F32)
    return lax.dot_general(
        ones, columns, (((1,), (1,)), ((), ())), precision=HIGHEST, preferred_element_type=F32
    )


def column_of(row, n):
    r = lax.broadcasted_iota(jnp.int32, (n, row.shape[1]), 0)
    c = lax.broadcasted_iota(jnp.int32, (n, row.shape[1]), 1)
    return jnp.sum(jnp.where(r == c, row, 0.0), axis=1, keepdims=True)


def row_of(column):
    n = column.shape[0]
    r = lax.broadcasted_iota(jnp.int32, (n, LANES), 0)
    c = lax.broadcasted_iota(jnp.int32, (n, LANES), 1)
    return jnp.sum(jnp.where(r == c, column, 0.0), axis=0, keepdims=True)


def sums_kernel(chunk, c_local, groups_of, relative, owner_hbm, assign_hbm, emb_hbm, *rest):
    outs, (owner, assign, emb, acc, cnt, sems) = rest[:-6], rest[-6:]
    n, feats = emb.shape
    cands = acc.shape[0]
    steps = n // chunk

    def copy(s):
        rows = pl.ds(s * chunk, chunk)
        return pltpu.make_async_copy(emb_hbm.at[rows], emb.at[rows], sems.at[s])

    owners = pltpu.make_async_copy(owner_hbm, owner, sems.at[steps])
    labels = pltpu.make_async_copy(assign_hbm, assign, sems.at[steps + 1])
    owners.start()
    for s in range(steps):
        copy(s).start()
    labels.start()
    row = lax.broadcasted_iota(jnp.int32, (cands, chunk), 0)
    owners.wait()
    for s in range(steps):
        hit = jnp.where(row == owner[:, s * chunk : (s + 1) * chunk], 1.0, 0.0)
        fold = hit[:, :LANES]
        for j in range(1, chunk // LANES):
            fold = fold + hit[:, j * LANES : (j + 1) * LANES]
        copy(s).wait()
        part = jnp.dot(
            hit.astype(jnp.bfloat16),
            emb[s * chunk : (s + 1) * chunk, :],
            preferred_element_type=F32,
        )
        if s == 0:
            acc[...] = part
            cnt[...] = fold
        else:
            acc[...] += part
            cnt[...] += fold
    labels.wait()
    me = lax.axis_index("dp")
    sub = c_local // SUBLANES
    for out, members in zip(outs, groups_of):
        for slot, k in enumerate(members):
            peer = me ^ k if relative else k
            base = peer * c_local
            dst = out.at[slot]
            for q in range(feats // LANES):
                for r in range(sub):
                    dst[q * sub + r] = acc[
                        pl.ds(pl.multiple_of(base + r * SUBLANES, SUBLANES), SUBLANES),
                        q * LANES : (q + 1) * LANES,
                    ]
            counts = lanes_of(cnt[pl.ds(pl.multiple_of(base, SUBLANES), c_local), :])
            rows = lax.broadcasted_iota(jnp.int32, counts.shape, 0)
            tile = dst.shape[0] - 1
            dst[tile] = jnp.zeros((SUBLANES, LANES), F32)
            dst[tile, :, :c_local] = jnp.where(rows == COUNT_ROW, counts, 0.0)
            if k == 0 or not relative:
                mine = assign[...].astype(F32)
                if not relative:
                    mine = jnp.where(me == k, mine, 0.0)
                dst[tile, LABEL_ROW : LABEL_ROW + mine.shape[0], :c_local] = mine


def partial_sums(embeddings, owner, assign, parts, groups_of, relative):
    n, feats = embeddings.shape
    c_local = assign.shape[1]
    chunk = min(512, n)
    tiles = (c_local // SUBLANES) * (feats // LANES) + 1
    operands = (owner.reshape(1, n), assign, embeddings)
    return pl.pallas_call(
        functools.partial(sums_kernel, chunk, c_local, groups_of, relative),
        out_shape=[
            jax.ShapeDtypeStruct((len(members), tiles, SUBLANES, LANES), F32)
            for members in groups_of
        ],
        in_specs=[pl.BlockSpec(memory_space=pltpu.HBM)] * 3,
        out_specs=[VMEM] * len(groups_of),
        scratch_shapes=[
            pltpu.VMEM((1, n), jnp.int32),
            pltpu.VMEM(assign.shape, jnp.int32),
            pltpu.VMEM((n, feats), embeddings.dtype),
            pltpu.VMEM((parts * c_local, feats), F32),
            pltpu.VMEM((parts * c_local, LANES), F32),
            pltpu.SemaphoreType.DMA((n // chunk + 2,)),
        ],
        compiler_params=pltpu.CompilerParams(vmem_limit_bytes=52 << 20),
        name="candidate_sums",
    )(*[pltpu.with_memory_space_constraint(x, pltpu.HBM) for x in operands])


def square_kernel(c_local, *refs):
    ins, out_ref, sq_ref = refs[:-2], refs[-2], refs[-1]
    slots = out_ref.shape[0]
    tiles = out_ref.shape[1] - 1
    sub = c_local // SUBLANES
    for slot in range(slots):
        blocks = [ins[0].at[slot]] + [ref.at[slots - 1 - slot] for ref in ins[1:]]
        squares = []
        for r in range(sub):
            total = None
            for q in range(tiles // sub):
                t = q * sub + r
                x = functools.reduce(jnp.add, [block[t] for block in blocks])
                out_ref[slot, t] = x
                total = x * x if total is None else total + x * x
            squares.append(total)
        out_ref[slot, tiles] = functools.reduce(jnp.add, [block[tiles] for block in blocks])
        lanes = lanes_of(jnp.concatenate(squares, axis=0))
        rows = lax.broadcasted_iota(jnp.int32, lanes.shape, 0)
        sq_ref[slot] = jnp.zeros(sq_ref.shape[1:], F32)
        sq_ref[slot, :, :c_local] = jnp.where(rows == SQUARE_ROW, lanes, 0.0)


def add_and_square(blocks, c_local):
    shape = blocks[0].shape
    return pl.pallas_call(
        functools.partial(square_kernel, c_local),
        out_shape=[
            jax.ShapeDtypeStruct(shape, F32),
            jax.ShapeDtypeStruct(shape[:1] + shape[2:], F32),
        ],
        in_specs=[VMEM] * len(blocks),
        out_specs=[VMEM] * 2,
        compiler_params=room(*[block.shape for block in blocks]),
        name="add_and_square",
    )(*blocks)


def totals_kernel(c_local, k_local, width, slot, own_pair, *refs):
    own_ref = own_pair.at[0]
    n_in = len(refs) - 4
    ins, (tot_ref, wgt_ref, q_ref, raw) = refs[:n_in], refs[n_in:]
    tiles = own_ref.shape[0] - 1
    groups = c_local // SUBLANES
    cols = tiles // groups
    steps = tot_ref.shape[0]
    views = []
    for ref in ins:
        views += [ref] if len(ref.shape) == 3 else [ref.at[j] for j in range(ref.shape[0])]
    per = LANES // slot
    aux = []
    for n, view in enumerate(views):
        for r in range(groups):
            at = n * slot + r * SUBLANES
            for q in range(cols):
                raw[at : at + SUBLANES, q * LANES : (q + 1) * LANES] = view[q * groups + r]
        if slot > c_local:
            raw[n * slot + c_local : (n + 1) * slot, :] = jnp.zeros(
                (slot - c_local, cols * LANES), F32
            )
        tile = view[tiles]
        if n % per == 0:
            aux.append(tile)
        else:
            aux[-1] = aux[-1] + pltpu.roll(tile, slot * (n % per), 1)
    aux = jnp.concatenate(aux, axis=1)
    lanes = aux.shape[1]
    if raw.shape[0] > len(views) * slot:
        raw[len(views) * slot :, :] = jnp.zeros((raw.shape[0] - len(views) * slot, cols * LANES), F32)
    count = aux[COUNT_ROW : COUNT_ROW + 1]
    scale = lax.rsqrt(aux[SQUARE_ROW : SQUARE_ROW + 1] / width + EPS)
    own_aux = own_ref[tiles]
    own_scale = lax.rsqrt(column_of(own_aux[SQUARE_ROW : SQUARE_ROW + 1], c_local) / width + EPS)
    first = lax.axis_index("dp") * k_local
    ids = (lax.broadcasted_iota(jnp.int32, (k_local, 1), 0) + first).astype(F32)
    picks, weights = [], []
    for t in range(steps):
        label = LABEL_ROW + t
        own = column_of(own_aux[label : label + 1], c_local)
        keys = jnp.concatenate([ids, own], axis=0)
        match = keys == aux[label : label + 1]
        picks.append(jnp.where(match, count * scale, 0.0))
        weights.append(jnp.sum(jnp.where(match, count, 0.0), axis=1, keepdims=True))
    total = jnp.dot(
        jnp.concatenate(picks, axis=0), raw[...], precision=HIGHEST, preferred_element_type=F32
    )
    means = jnp.concatenate(
        [
            jnp.concatenate([own_ref[q * groups + r] for q in range(cols)], axis=1)
            for r in range(groups)
        ],
        axis=0,
    ) * own_scale
    span = k_local + c_local
    lane = lax.broadcasted_iota(jnp.int32, (c_local, LANES), 1)
    lane_k = lax.broadcasted_iota(jnp.int32, (k_local, LANES), 1)
    q_c = jnp.zeros((c_local, LANES), F32)
    q_k = jnp.zeros((k_local, LANES), F32)
    w_c = jnp.zeros((c_local, LANES), F32)
    w_k = jnp.zeros((k_local, LANES), F32)
    for t in range(steps):
        t_k = total[t * span : t * span + k_local]
        t_c = total[t * span + k_local : (t + 1) * span]
        weight = weights[t]
        near = weight[k_local:]
        center = t_c / jnp.where(near > 0, near, 1.0)
        diff = means - center
        for j, (a, b) in enumerate(((diff, diff), (diff, center), (center, center))):
            q_c = jnp.where(lane == 4 * t + j, jnp.sum(a * b, axis=1, keepdims=True), q_c)
        q_k = jnp.where(lane_k == t, jnp.sum(t_k * t_k, axis=1, keepdims=True), q_k)
        w_c = jnp.where(lane == t, near, w_c)
        w_k = jnp.where(lane_k == t, weight[:k_local], w_k)
        tot_ref[t] = t_k
    q_ref[:c_local] = q_c
    q_ref[c_local:] = q_k
    wgt_ref[:c_local] = w_c
    wgt_ref[c_local:] = w_k


def totals(own, ins, steps, parts, c_local, k_local, feats, width):
    slot = 8
    while slot < c_local:
        slot *= 2
    lanes = -(-parts * slot // LANES) * LANES
    rows = c_local + k_local
    return pl.pallas_call(
        functools.partial(totals_kernel, c_local, k_local, width, slot),
        out_shape=[
            jax.ShapeDtypeStruct((steps, k_local, feats), F32),
            jax.ShapeDtypeStruct((rows, LANES), F32),
            jax.ShapeDtypeStruct((rows, LANES), F32),
        ],
        in_specs=[VMEM] * (1 + len(ins)),
        out_specs=[VMEM] * 3,
        scratch_shapes=[pltpu.VMEM((lanes, feats), F32)],
        compiler_params=room((lanes, 2 * feats)),
        name="cluster_totals",
    )(own, *ins)


def finish_kernel(c_local, width, tot_ref, wgt_ref, q_ref, init_ref, cen_ref, spread_ref):
    steps = tot_ref.shape[0]
    current = init_ref[...]
    for t in range(steps):
        length = q_ref[c_local:, t : t + 1]
        fresh = tot_ref[t] * lax.rsqrt(length / width + EPS)
        current = jnp.where(wgt_ref[c_local:, t : t + 1] > 0, fresh, current)
        near = wgt_ref[:c_local, t : t + 1]
        dd, da, aa = (q_ref[:c_local, 4 * t + j : 4 * t + j + 1] for j in range(3))
        gap = 1.0 - near * lax.rsqrt(near * near * (aa / width) + EPS)
        spread = (dd + gap * (2.0 * da + gap * aa)) / width
        spread_ref[t : t + 1, :] = row_of(spread)[:, :c_local]
    cen_ref[...] = current


def finish(tot, wgt, q, init, c_local, width):
    return pl.pallas_call(
        functools.partial(finish_kernel, c_local, width),
        out_shape=[
            jax.ShapeDtypeStruct(init.shape, F32),
            jax.ShapeDtypeStruct((tot.shape[0], c_local), F32),
        ],
        in_specs=[VMEM] * 4,
        out_specs=[VMEM] * 2,
        compiler_params=room(tot.shape, init.shape),
        name="finish",
    )(tot, wgt, q, init)


def per_device(embeddings, sample_owner, lloyd_assign, init_centroids):
    parts = lax.axis_size("dp")
    steps, c_local = lloyd_assign.shape
    k_local, feats = init_centroids.shape
    width = feats * lax.axis_size("feat")
    top = parts // 2
    direct = 2 <= parts <= 16 and parts & (parts - 1) == 0
    if direct:
        groups_of = [(k, k ^ top) for k in range(top)]
    else:
        groups_of = [tuple(range(parts))]
    blocks = partial_sums(embeddings, sample_owner, lloyd_assign, parts, groups_of, direct)
    if direct:
        near = [swap(blocks[k], "dp", parts, k) for k in reversed(range(1, top))]
        pair = functools.reduce(jnp.add, near, blocks[0])
        blocks = [pair, swap(pair, "dp", parts, top)]
    else:
        blocks = [lax.psum_scatter(blocks[0], "dp", scatter_dimension=0)[None]]
    own, squares = add_and_square(blocks, c_local)
    own = own.at[:, -1].add(sum_over(squares, "feat"))
    if direct:
        everyone = [own] + [swap(own, "dp", parts, k) for k in reversed(range(1, top))]
    else:
        everyone = [lax.all_gather(own[0], "dp")]
    tot, wgt, q = totals(own, everyone, steps, parts, c_local, k_local, feats, width)
    q = sum_over(q, "feat")
    centroids, spread = finish(tot, wgt, q, init_centroids, c_local, width)
    return centroids, spread


def solution(mesh):
    in_specs = (P("dp", "feat"), P("dp"), P(None, "dp"), P("dp", "feat"))
    out_specs = (P("dp", "feat"), P(None, "dp"))
    return jax.shard_map(
        per_device, mesh=mesh, in_specs=in_specs, out_specs=out_specs, check_vma=False
    )
```

```python
import functools
import math

import jax
import jax.numpy as jnp
from jax import lax
from jax.experimental import pallas as pl
from jax.experimental.pallas import tpu as pltpu
from jax.sharding import PartitionSpec as P

EPS = 1e-06
LANES = 128
SUBLANES = 8
COUNT_ROW, SQUARE_ROW, LABEL_ROW = 0, 1, 2
HIGHEST = lax.Precision.HIGHEST
F32 = jnp.float32
VMEM = pl.BlockSpec(memory_space=pltpu.VMEM)


def room(*arrays):
    held = sum(4 * math.prod(shape) for shape in arrays)
    return pltpu.CompilerParams(vmem_limit_bytes=min((8 << 20) + 2 * held, 60 << 20))


def swap(x, axis, size, k):
    return lax.ppermute(x, axis, [(i, i ^ k) for i in range(size)])


def sum_over(x, axis):
    size = lax.axis_size(axis)
    if size & (size - 1) or size > 4:
        return lax.psum(x, axis)
    parts = [swap(x, axis, size, k) for k in range(1, size)]
    return functools.reduce(jnp.add, parts, x)


def lanes_of(columns, small=False):
    kind = jnp.bfloat16 if small else F32
    return lax.dot_general(
        jnp.ones((SUBLANES, columns.shape[1]), kind),
        columns.astype(kind),
        (((1,), (1,)), ((), ())),
        precision=None if small else HIGHEST,
        preferred_element_type=F32,
    )


def column_of(row, n):
    r = lax.broadcasted_iota(jnp.int32, (n, row.shape[1]), 0)
    c = lax.broadcasted_iota(jnp.int32, (n, row.shape[1]), 1)
    return jnp.sum(jnp.where(r == c, row, 0.0), axis=1, keepdims=True)


def row_of(column):
    n = column.shape[0]
    r = lax.broadcasted_iota(jnp.int32, (n, LANES), 0)
    c = lax.broadcasted_iota(jnp.int32, (n, LANES), 1)
    return jnp.sum(jnp.where(r == c, column, 0.0), axis=0, keepdims=True)


def sums_kernel(chunks, c_local, groups_of, relative, owner_hbm, assign_hbm, emb_hbm, *rest):
    outs, (owner, assign, emb, acc, cnt, sems) = rest[:-6], rest[-6:]
    n, feats = emb.shape
    cands = acc.shape[0]
    steps = len(chunks)
    starts = [sum(chunks[:s]) for s in range(steps)]

    def copy(s):
        rows = pl.ds(starts[s], chunks[s])
        return pltpu.make_async_copy(emb_hbm.at[rows], emb.at[rows], sems.at[s])

    owners = pltpu.make_async_copy(owner_hbm, owner, sems.at[steps])
    labels = pltpu.make_async_copy(assign_hbm, assign, sems.at[steps + 1])
    owners.start()
    for s in range(steps):
        copy(s).start()
    labels.start()
    owners.wait()
    for s, (start, chunk) in enumerate(zip(starts, chunks)):
        row = lax.broadcasted_iota(jnp.int32, (cands, chunk), 0)
        hit = jnp.where(row == owner[:, start : start + chunk], 1.0, 0.0)
        fold = hit[:, :LANES]
        for j in range(1, chunk // LANES):
            fold = fold + hit[:, j * LANES : (j + 1) * LANES]
        copy(s).wait()
        part = jnp.dot(
            hit.astype(jnp.bfloat16),
            emb[start : start + chunk, :],
            preferred_element_type=F32,
        )
        if s == 0:
            acc[...] = part
            cnt[...] = fold
        else:
            acc[...] += part
            cnt[...] += fold
    labels.wait()
    me = lax.axis_index("dp")
    sub = c_local // SUBLANES
    counts = lanes_of(cnt[...], n <= 256 * LANES)
    if cands % LANES:
        blank = jnp.zeros((SUBLANES, LANES - cands % LANES), F32)
        counts = jnp.concatenate([counts, blank], axis=1)
    for out, members in zip(outs, groups_of):
        for slot, k in enumerate(members):
            peer = me ^ k if relative else k
            base = peer * c_local
            dst = out.at[slot]
            for q in range(feats // LANES):
                for r in range(sub):
                    dst[q * sub + r] = acc[
                        pl.ds(pl.multiple_of(base + r * SUBLANES, SUBLANES), SUBLANES),
                        q * LANES : (q + 1) * LANES,
                    ]
            mine = pltpu.roll(counts, lax.rem(counts.shape[1] - base, counts.shape[1]), 1)
            mine = mine[:, :c_local]
            rows = lax.broadcasted_iota(jnp.int32, mine.shape, 0)
            tile = dst.shape[0] - 1
            dst[tile] = jnp.zeros((SUBLANES, LANES), F32)
            dst[tile, :, :c_local] = jnp.where(rows == COUNT_ROW, mine, 0.0)
            if k == 0 or not relative:
                own = assign[...].astype(F32)
                if not relative:
                    own = jnp.where(me == k, own, 0.0)
                dst[tile, LABEL_ROW : LABEL_ROW + own.shape[0], :c_local] = own


def chunks_of(n):
    quarter = n // 4
    if quarter % (4 * LANES):
        return [LANES] * (n // LANES)
    return [quarter] * 3 + [quarter // 2, quarter // 4, quarter // 4]


def partial_sums(embeddings, owner, assign, parts, groups_of, relative):
    n, feats = embeddings.shape
    c_local = assign.shape[1]
    chunks = chunks_of(n)
    tiles = (c_local // SUBLANES) * (feats // LANES) + 1
    operands = (owner.reshape(1, n), assign, embeddings)
    return pl.pallas_call(
        functools.partial(sums_kernel, chunks, c_local, groups_of, relative),
        out_shape=[
            jax.ShapeDtypeStruct((len(members), tiles, SUBLANES, LANES), F32)
            for members in groups_of
        ],
        in_specs=[pl.BlockSpec(memory_space=pltpu.HBM)] * 3,
        out_specs=[VMEM] * len(groups_of),
        scratch_shapes=[
            pltpu.VMEM((1, n), jnp.int32),
            pltpu.VMEM(assign.shape, jnp.int32),
            pltpu.VMEM((n, feats), embeddings.dtype),
            pltpu.VMEM((parts * c_local, feats), F32),
            pltpu.VMEM((parts * c_local, LANES), F32),
            pltpu.SemaphoreType.DMA((len(chunks) + 2,)),
        ],
        compiler_params=pltpu.CompilerParams(vmem_limit_bytes=52 << 20),
        name="candidate_sums",
    )(*[pltpu.with_memory_space_constraint(x, pltpu.HBM) for x in operands])


def square_kernel(c_local, *refs):
    ins, out_ref, sq_ref = refs[:-2], refs[-2], refs[-1]
    slots = out_ref.shape[0]
    tiles = out_ref.shape[1] - 1
    sub = c_local // SUBLANES
    for slot in range(slots):
        blocks = [ins[0].at[slot]] + [ref.at[slots - 1 - slot] for ref in ins[1:]]
        squares = []
        for r in range(sub):
            total = None
            for q in range(tiles // sub):
                t = q * sub + r
                x = functools.reduce(jnp.add, [block[t] for block in blocks])
                out_ref[slot, t] = x
                total = x * x if total is None else total + x * x
            squares.append(total)
        out_ref[slot, tiles] = functools.reduce(jnp.add, [block[tiles] for block in blocks])
        lanes = lanes_of(jnp.concatenate(squares, axis=0))
        rows = lax.broadcasted_iota(jnp.int32, lanes.shape, 0)
        sq_ref[slot] = jnp.zeros(sq_ref.shape[1:], F32)
        sq_ref[slot, :, :c_local] = jnp.where(rows == SQUARE_ROW, lanes, 0.0)


def add_and_square(blocks, c_local):
    shape = blocks[0].shape
    return pl.pallas_call(
        functools.partial(square_kernel, c_local),
        out_shape=[
            jax.ShapeDtypeStruct(shape, F32),
            jax.ShapeDtypeStruct(shape[:1] + shape[2:], F32),
        ],
        in_specs=[VMEM] * len(blocks),
        out_specs=[VMEM] * 2,
        compiler_params=room(*[block.shape for block in blocks]),
        name="add_and_square",
    )(*blocks)


def totals_kernel(c_local, k_local, width, slot, own_pair, *refs):
    own_ref = own_pair.at[0]
    n_in = len(refs) - 4
    ins, (tot_ref, wgt_ref, q_ref, raw) = refs[:n_in], refs[n_in:]
    tiles = own_ref.shape[0] - 1
    groups = c_local // SUBLANES
    cols = tiles // groups
    steps = tot_ref.shape[0]
    views = []
    for ref in ins:
        views += [ref] if len(ref.shape) == 3 else [ref.at[j] for j in range(ref.shape[0])]
    per = LANES // slot
    aux = []
    for n, view in enumerate(views):
        for r in range(groups):
            at = n * slot + r * SUBLANES
            for q in range(cols):
                raw[at : at + SUBLANES, q * LANES : (q + 1) * LANES] = view[q * groups + r]
        if slot > c_local:
            raw[n * slot + c_local : (n + 1) * slot, :] = jnp.zeros(
                (slot - c_local, cols * LANES), F32
            )
        tile = view[tiles]
        if n % per == 0:
            aux.append(tile)
        else:
            aux[-1] = aux[-1] + pltpu.roll(tile, slot * (n % per), 1)
    aux = jnp.concatenate(aux, axis=1)
    lanes = aux.shape[1]
    if raw.shape[0] > len(views) * slot:
        raw[len(views) * slot :, :] = jnp.zeros((raw.shape[0] - len(views) * slot, cols * LANES), F32)
    count = aux[COUNT_ROW : COUNT_ROW + 1]
    scale = lax.rsqrt(aux[SQUARE_ROW : SQUARE_ROW + 1] / width + EPS)
    own_aux = own_ref[tiles]
    own_scale = lax.rsqrt(column_of(own_aux[SQUARE_ROW : SQUARE_ROW + 1], c_local) / width + EPS)
    first = lax.axis_index("dp") * k_local
    ids = (lax.broadcasted_iota(jnp.int32, (k_local, 1), 0) + first).astype(F32)
    picks, weights = [], []
    for t in range(steps):
        label = LABEL_ROW + t
        own = column_of(own_aux[label : label + 1], c_local)
        keys = jnp.concatenate([ids, own], axis=0)
        match = keys == aux[label : label + 1]
        picks.append(jnp.where(match, count * scale, 0.0))
        weights.append(jnp.sum(jnp.where(match, count, 0.0), axis=1, keepdims=True))
    total = jnp.dot(
        jnp.concatenate(picks, axis=0), raw[...], precision=HIGHEST, preferred_element_type=F32
    )
    means = jnp.concatenate(
        [
            jnp.concatenate([own_ref[q * groups + r] for q in range(cols)], axis=1)
            for r in range(groups)
        ],
        axis=0,
    ) * own_scale
    span = k_local + c_local
    lane = lax.broadcasted_iota(jnp.int32, (c_local, LANES), 1)
    lane_k = lax.broadcasted_iota(jnp.int32, (k_local, LANES), 1)
    q_c = jnp.zeros((c_local, LANES), F32)
    q_k = jnp.zeros((k_local, LANES), F32)
    w_c = jnp.zeros((c_local, LANES), F32)
    w_k = jnp.zeros((k_local, LANES), F32)
    for t in range(steps):
        t_k = total[t * span : t * span + k_local]
        t_c = total[t * span + k_local : (t + 1) * span]
        weight = weights[t]
        near = weight[k_local:]
        center = t_c / jnp.where(near > 0, near, 1.0)
        diff = means - center
        for j, (a, b) in enumerate(((diff, diff), (diff, center), (center, center))):
            q_c = jnp.where(lane == 4 * t + j, jnp.sum(a * b, axis=1, keepdims=True), q_c)
        q_k = jnp.where(lane_k == t, jnp.sum(t_k * t_k, axis=1, keepdims=True), q_k)
        w_c = jnp.where(lane == t, near, w_c)
        w_k = jnp.where(lane_k == t, weight[:k_local], w_k)
        tot_ref[t] = t_k
    q_ref[:c_local] = q_c
    q_ref[c_local:] = q_k
    wgt_ref[:c_local] = w_c
    wgt_ref[c_local:] = w_k


def totals(own, ins, steps, parts, c_local, k_local, feats, width):
    slot = 8
    while slot < c_local:
        slot *= 2
    lanes = -(-parts * slot // LANES) * LANES
    rows = c_local + k_local
    return pl.pallas_call(
        functools.partial(totals_kernel, c_local, k_local, width, slot),
        out_shape=[
            jax.ShapeDtypeStruct((steps, k_local, feats), F32),
            jax.ShapeDtypeStruct((rows, LANES), F32),
            jax.ShapeDtypeStruct((rows, LANES), F32),
        ],
        in_specs=[VMEM] * (1 + len(ins)),
        out_specs=[VMEM] * 3,
        scratch_shapes=[pltpu.VMEM((lanes, feats), F32)],
        compiler_params=room((lanes, 2 * feats)),
        name="cluster_totals",
    )(own, *ins)


def finish_kernel(c_local, width, tot_ref, wgt_ref, q_ref, init_ref, cen_ref, spread_ref):
    steps = tot_ref.shape[0]
    current = init_ref[...]
    for t in range(steps):
        length = q_ref[c_local:, t : t + 1]
        fresh = tot_ref[t] * lax.rsqrt(length / width + EPS)
        current = jnp.where(wgt_ref[c_local:, t : t + 1] > 0, fresh, current)
        near = wgt_ref[:c_local, t : t + 1]
        dd, da, aa = (q_ref[:c_local, 4 * t + j : 4 * t + j + 1] for j in range(3))
        gap = 1.0 - near * lax.rsqrt(near * near * (aa / width) + EPS)
        spread = (dd + gap * (2.0 * da + gap * aa)) / width
        spread_ref[t : t + 1, :] = row_of(spread)[:, :c_local]
    cen_ref[...] = current


def finish(tot, wgt, q, init, c_local, width):
    return pl.pallas_call(
        functools.partial(finish_kernel, c_local, width),
        out_shape=[
            jax.ShapeDtypeStruct(init.shape, F32),
            jax.ShapeDtypeStruct((tot.shape[0], c_local), F32),
        ],
        in_specs=[VMEM] * 4,
        out_specs=[VMEM] * 2,
        compiler_params=room(tot.shape, init.shape),
        name="finish",
    )(tot, wgt, q, init)


def per_device(embeddings, sample_owner, lloyd_assign, init_centroids):
    parts = lax.axis_size("dp")
    steps, c_local = lloyd_assign.shape
    k_local, feats = init_centroids.shape
    width = feats * lax.axis_size("feat")
    top = parts // 2
    direct = 2 <= parts <= 16 and parts & (parts - 1) == 0
    if direct:
        groups_of = [(k, k ^ top) for k in range(top)]
    else:
        groups_of = [tuple(range(parts))]
    blocks = partial_sums(embeddings, sample_owner, lloyd_assign, parts, groups_of, direct)
    if direct:
        near = [swap(blocks[k], "dp", parts, k) for k in (1, 3, 2)]
        pair = functools.reduce(jnp.add, near, blocks[0])
        blocks = [pair, swap(pair, "dp", parts, top)]
    else:
        blocks = [lax.psum_scatter(blocks[0], "dp", scatter_dimension=0)[None]]
    own, squares = add_and_square(blocks, c_local)
    own = own.at[:, -1].add(sum_over(squares, "feat"))
    if direct:
        everyone = [own] + [swap(own, "dp", parts, k) for k in range(1, top)]
    else:
        everyone = [lax.all_gather(own[0], "dp")]
    tot, wgt, q = totals(own, everyone, steps, parts, c_local, k_local, feats, width)
    q = sum_over(q, "feat")
    centroids, spread = finish(tot, wgt, q, init_centroids, c_local, width)
    return centroids, spread


def solution(mesh):
    in_specs = (P("dp", "feat"), P("dp"), P(None, "dp"), P("dp", "feat"))
    out_specs = (P("dp", "feat"), P(None, "dp"))
    return jax.shard_map(
        per_device, mesh=mesh, in_specs=in_specs, out_specs=out_specs, check_vma=False
    )
```

```python
import functools
import math

import jax
import jax.numpy as jnp
from jax import lax
from jax.experimental import pallas as pl
from jax.experimental.pallas import tpu as pltpu
from jax.sharding import PartitionSpec as P

EPS = 1e-06
LANES = 128
SUBLANES = 8
COUNT_ROW, SQUARE_ROW, LABEL_ROW = 0, 1, 2
SLOT_ROWS = 4
HIGHEST = lax.Precision.HIGHEST
F32 = jnp.float32
VMEM = pl.BlockSpec(memory_space=pltpu.VMEM)


def room(*arrays):
    held = sum(4 * math.prod(shape) for shape in arrays)
    return pltpu.CompilerParams(vmem_limit_bytes=min((8 << 20) + 2 * held, 60 << 20))


def swap(x, axis, size, k):
    return lax.ppermute(x, axis, [(i, i ^ k) for i in range(size)])


def sum_over(x, axis):
    size = lax.axis_size(axis)
    if size & (size - 1) or size > 4:
        return lax.psum(x, axis)
    parts = [swap(x, axis, size, k) for k in range(1, size)]
    return functools.reduce(jnp.add, parts, x)


def lanes_of(columns, small=False):
    kind = jnp.bfloat16 if small else F32
    return lax.dot_general(
        jnp.ones((SUBLANES, columns.shape[1]), kind),
        columns.astype(kind),
        (((1,), (1,)), ((), ())),
        precision=None if small else HIGHEST,
        preferred_element_type=F32,
    )


def column_of(row, n):
    r = lax.broadcasted_iota(jnp.int32, (n, row.shape[1]), 0)
    c = lax.broadcasted_iota(jnp.int32, (n, row.shape[1]), 1)
    return jnp.sum(jnp.where(r == c, row, 0.0), axis=1, keepdims=True)


def row_of(column):
    n = column.shape[0]
    r = lax.broadcasted_iota(jnp.int32, (n, LANES), 0)
    c = lax.broadcasted_iota(jnp.int32, (n, LANES), 1)
    return jnp.sum(jnp.where(r == c, column, 0.0), axis=0, keepdims=True)


def sums_kernel(chunks, c_local, groups_of, relative, owner_hbm, assign_hbm, emb_hbm, *rest):
    outs, (owner, assign, emb, acc, cnt, sems) = rest[:-6], rest[-6:]
    n, feats = emb.shape
    cands = acc.shape[0]
    steps = len(chunks)
    starts = [sum(chunks[:s]) for s in range(steps)]

    def copy(s):
        rows = pl.ds(starts[s], chunks[s])
        return pltpu.make_async_copy(emb_hbm.at[rows], emb.at[rows], sems.at[s])

    owners = pltpu.make_async_copy(owner_hbm, owner, sems.at[steps])
    labels = pltpu.make_async_copy(assign_hbm, assign, sems.at[steps + 1])
    owners.start()
    for s in range(steps):
        copy(s).start()
    labels.start()
    owners.wait()
    for s, (start, chunk) in enumerate(zip(starts, chunks)):
        row = lax.broadcasted_iota(jnp.int32, (cands, chunk), 0)
        hit = jnp.where(row == owner[:, start : start + chunk], 1.0, 0.0)
        fold = hit[:, :LANES]
        for j in range(1, chunk // LANES):
            fold = fold + hit[:, j * LANES : (j + 1) * LANES]
        copy(s).wait()
        part = jnp.dot(
            hit.astype(jnp.bfloat16),
            emb[start : start + chunk, :],
            preferred_element_type=F32,
        )
        if s == 0:
            acc[...] = part
            cnt[...] = fold
        else:
            acc[...] += part
            cnt[...] += fold
    labels.wait()
    me = lax.axis_index("dp")
    sub = c_local // SUBLANES
    counts = lanes_of(cnt[...], n <= 256 * LANES)
    if cands % LANES:
        blank = jnp.zeros((SUBLANES, LANES - cands % LANES), F32)
        counts = jnp.concatenate([counts, blank], axis=1)
    tiles = sub * (feats // LANES)
    for out, members in zip(outs, groups_of):
        for slot, k in enumerate(members):
            peer = me ^ k if relative else k
            base = peer * c_local
            dst, at = (out, slot) if relative else (out.at[slot], 0)
            for q in range(feats // LANES):
                for r in range(sub):
                    dst[at * tiles + q * sub + r] = acc[
                        pl.ds(pl.multiple_of(base + r * SUBLANES, SUBLANES), SUBLANES),
                        q * LANES : (q + 1) * LANES,
                    ]
            if at == 0:
                dst[dst.shape[0] - 1] = jnp.zeros((SUBLANES, LANES), F32)
            mine = pltpu.roll(counts, lax.rem(counts.shape[1] - base, counts.shape[1]), 1)
            row = at * SLOT_ROWS + COUNT_ROW
            dst[dst.shape[0] - 1, row : row + 1, :c_local] = mine[:1, :c_local]
            if k == 0 or not relative:
                own = assign[...].astype(F32)
                if not relative:
                    own = jnp.where(me == k, own, 0.0)
                dst[dst.shape[0] - 1, LABEL_ROW : LABEL_ROW + own.shape[0], :c_local] = own


def chunks_of(n):
    quarter = n // 4
    if quarter % (4 * LANES):
        return [LANES] * (n // LANES)
    return [quarter] * 3 + [quarter // 2, quarter // 4, quarter // 4]


def partial_sums(embeddings, owner, assign, parts, groups_of, relative):
    n, feats = embeddings.shape
    c_local = assign.shape[1]
    chunks = chunks_of(n)
    tiles = (c_local // SUBLANES) * (feats // LANES)
    shapes = [
        (len(members) * tiles + 1,) if relative else (len(members), tiles + 1)
        for members in groups_of
    ]
    operands = (owner.reshape(1, n), assign, embeddings)
    return pl.pallas_call(
        functools.partial(sums_kernel, chunks, c_local, groups_of, relative),
        out_shape=[jax.ShapeDtypeStruct((*shape, SUBLANES, LANES), F32) for shape in shapes],
        in_specs=[pl.BlockSpec(memory_space=pltpu.HBM)] * 3,
        out_specs=[VMEM] * len(groups_of),
        scratch_shapes=[
            pltpu.VMEM((1, n), jnp.int32),
            pltpu.VMEM(assign.shape, jnp.int32),
            pltpu.VMEM((n, feats), embeddings.dtype),
            pltpu.VMEM((parts * c_local, feats), F32),
            pltpu.VMEM((parts * c_local, LANES), F32),
            pltpu.SemaphoreType.DMA((len(chunks) + 2,)),
        ],
        compiler_params=pltpu.CompilerParams(vmem_limit_bytes=52 << 20),
        name="candidate_sums",
    )(*[pltpu.with_memory_space_constraint(x, pltpu.HBM) for x in operands])


def other_slot(tile):
    return jnp.concatenate([tile[SLOT_ROWS:], tile[:SLOT_ROWS]], axis=0)


def square_kernel(c_local, slots, *refs):
    ins, out_ref, sq_ref = refs[:-2], refs[-2], refs[-1]
    last = out_ref.shape[0] - 1
    tiles = last // slots
    sub = c_local // SUBLANES
    sq_ref[...] = jnp.zeros_like(sq_ref)
    for slot in range(slots):
        squares = []
        for r in range(sub):
            total = None
            for q in range(tiles // sub):
                t = q * sub + r
                x = ins[0][slot * tiles + t]
                if len(ins) > 1:
                    x = x + ins[1][(slots - 1 - slot) * tiles + t]
                out_ref[slot * tiles + t] = x
                total = x * x if total is None else total + x * x
            squares.append(total)
        lanes = lanes_of(jnp.concatenate(squares, axis=0))
        row = slot * SLOT_ROWS + SQUARE_ROW
        sq_ref[row : row + 1, :c_local] = lanes[:1]
    aux = ins[0][last]
    out_ref[last] = aux + other_slot(ins[1][last]) if len(ins) > 1 else aux


def add_and_square(blocks, c_local, slots):
    shape = blocks[0].shape
    return pl.pallas_call(
        functools.partial(square_kernel, c_local, slots),
        out_shape=[
            jax.ShapeDtypeStruct(shape, F32),
            jax.ShapeDtypeStruct(shape[1:], F32),
        ],
        in_specs=[VMEM] * len(blocks),
        out_specs=[VMEM] * 2,
        compiler_params=room(*[block.shape for block in blocks]),
        name="add_and_square",
    )(*blocks)


def totals_kernel(c_local, k_local, width, slot, cols, own_ref, *refs):
    n_in = len(refs) - 4
    ins, (tot_ref, wgt_ref, q_ref, raw) = refs[:n_in], refs[n_in:]
    groups = c_local // SUBLANES
    tiles = groups * cols
    steps = tot_ref.shape[0]
    views = []
    for ref in ins:
        if len(ref.shape) == 4:
            views += [(ref.at[j], 0) for j in range(ref.shape[0])]
        else:
            views += [(ref, j) for j in range(ref.shape[0] // tiles)]
    per = LANES // slot
    aux = []
    for n, (view, j) in enumerate(views):
        for r in range(groups):
            at = n * slot + r * SUBLANES
            for q in range(cols):
                raw[at : at + SUBLANES, q * LANES : (q + 1) * LANES] = view[
                    j * tiles + q * groups + r
                ]
        if slot > c_local:
            raw[n * slot + c_local : (n + 1) * slot, :] = jnp.zeros(
                (slot - c_local, cols * LANES), F32
            )
        tile = view[view.shape[0] - 1]
        if j:
            tile = other_slot(tile)
        if n % per == 0:
            aux.append(tile)
        else:
            aux[-1] = aux[-1] + pltpu.roll(tile, slot * (n % per), 1)
    aux = jnp.concatenate(aux, axis=1)
    lanes = aux.shape[1]
    if raw.shape[0] > len(views) * slot:
        raw[len(views) * slot :, :] = jnp.zeros((raw.shape[0] - len(views) * slot, cols * LANES), F32)
    count = aux[COUNT_ROW : COUNT_ROW + 1]
    scale = lax.rsqrt(aux[SQUARE_ROW : SQUARE_ROW + 1] / width + EPS)
    own_aux = own_ref[own_ref.shape[0] - 1]
    own_scale = lax.rsqrt(column_of(own_aux[SQUARE_ROW : SQUARE_ROW + 1], c_local) / width + EPS)
    first = lax.axis_index("dp") * k_local
    ids = (lax.broadcasted_iota(jnp.int32, (k_local, 1), 0) + first).astype(F32)
    picks, weights = [], []
    for t in range(steps):
        label = LABEL_ROW + t
        own = column_of(own_aux[label : label + 1], c_local)
        keys = jnp.concatenate([ids, own], axis=0)
        match = keys == aux[label : label + 1]
        picks.append(jnp.where(match, count * scale, 0.0))
        weights.append(jnp.sum(jnp.where(match, count, 0.0), axis=1, keepdims=True))
    total = jnp.dot(
        jnp.concatenate(picks, axis=0), raw[...], precision=HIGHEST, preferred_element_type=F32
    )
    means = jnp.concatenate(
        [
            jnp.concatenate([own_ref[q * groups + r] for q in range(cols)], axis=1)
            for r in range(groups)
        ],
        axis=0,
    ) * own_scale
    span = k_local + c_local
    lane = lax.broadcasted_iota(jnp.int32, (c_local, LANES), 1)
    lane_k = lax.broadcasted_iota(jnp.int32, (k_local, LANES), 1)
    q_c = jnp.zeros((c_local, LANES), F32)
    q_k = jnp.zeros((k_local, LANES), F32)
    w_c = jnp.zeros((c_local, LANES), F32)
    w_k = jnp.zeros((k_local, LANES), F32)
    for t in range(steps):
        t_k = total[t * span : t * span + k_local]
        t_c = total[t * span + k_local : (t + 1) * span]
        weight = weights[t]
        near = weight[k_local:]
        center = t_c / jnp.where(near > 0, near, 1.0)
        diff = means - center
        for j, (a, b) in enumerate(((diff, diff), (diff, center), (center, center))):
            q_c = jnp.where(lane == 4 * t + j, jnp.sum(a * b, axis=1, keepdims=True), q_c)
        q_k = jnp.where(lane_k == t, jnp.sum(t_k * t_k, axis=1, keepdims=True), q_k)
        w_c = jnp.where(lane == t, near, w_c)
        w_k = jnp.where(lane_k == t, weight[:k_local], w_k)
        tot_ref[t] = t_k
    q_ref[:c_local] = q_c
    q_ref[c_local:] = q_k
    wgt_ref[:c_local] = w_c
    wgt_ref[c_local:] = w_k


def totals(own, ins, steps, parts, c_local, k_local, feats, width):
    slot = 8
    while slot < c_local:
        slot *= 2
    lanes = -(-parts * slot // LANES) * LANES
    rows = c_local + k_local
    return pl.pallas_call(
        functools.partial(totals_kernel, c_local, k_local, width, slot, feats // LANES),
        out_shape=[
            jax.ShapeDtypeStruct((steps, k_local, feats), F32),
            jax.ShapeDtypeStruct((rows, LANES), F32),
            jax.ShapeDtypeStruct((rows, LANES), F32),
        ],
        in_specs=[VMEM] * (1 + len(ins)),
        out_specs=[VMEM] * 3,
        scratch_shapes=[pltpu.VMEM((lanes, feats), F32)],
        compiler_params=room((lanes, 2 * feats)),
        name="cluster_totals",
    )(own, *ins)


def finish_kernel(c_local, width, tot_ref, wgt_ref, q_ref, init_ref, cen_ref, spread_ref):
    steps = tot_ref.shape[0]
    current = init_ref[...]
    for t in range(steps):
        length = q_ref[c_local:, t : t + 1]
        fresh = tot_ref[t] * lax.rsqrt(length / width + EPS)
        current = jnp.where(wgt_ref[c_local:, t : t + 1] > 0, fresh, current)
        near = wgt_ref[:c_local, t : t + 1]
        dd, da, aa = (q_ref[:c_local, 4 * t + j : 4 * t + j + 1] for j in range(3))
        gap = 1.0 - near * lax.rsqrt(near * near * (aa / width) + EPS)
        spread = (dd + gap * (2.0 * da + gap * aa)) / width
        spread_ref[t : t + 1, :] = row_of(spread)[:, :c_local]
    cen_ref[...] = current


def finish(tot, wgt, q, init, c_local, width):
    return pl.pallas_call(
        functools.partial(finish_kernel, c_local, width),
        out_shape=[
            jax.ShapeDtypeStruct(init.shape, F32),
            jax.ShapeDtypeStruct((tot.shape[0], c_local), F32),
        ],
        in_specs=[VMEM] * 4,
        out_specs=[VMEM] * 2,
        compiler_params=room(tot.shape, init.shape),
        name="finish",
    )(tot, wgt, q, init)


def per_device(embeddings, sample_owner, lloyd_assign, init_centroids):
    parts = lax.axis_size("dp")
    steps, c_local = lloyd_assign.shape
    assert LABEL_ROW + steps <= SLOT_ROWS
    k_local, feats = init_centroids.shape
    width = feats * lax.axis_size("feat")
    top = parts // 2
    direct = 2 <= parts <= 16 and parts & (parts - 1) == 0
    order = sorted(range(1, top), key=lambda k: (k.bit_count(), -k))
    if direct:
        groups_of = [(k, k ^ top) for k in range(top)]
    else:
        groups_of = [tuple(range(parts))]
    blocks = partial_sums(embeddings, sample_owner, lloyd_assign, parts, groups_of, direct)
    if direct:
        near = [swap(blocks[k], "dp", parts, k) for k in order]
        pair = functools.reduce(jnp.add, near, blocks[0])
        blocks = [pair, swap(pair, "dp", parts, top)]
    else:
        blocks = [lax.psum_scatter(blocks[0], "dp", scatter_dimension=0)]
    own, squares = add_and_square(blocks, c_local, 2 if direct else 1)
    own = own.at[-1].add(sum_over(squares, "feat"))
    if direct:
        everyone = [own] + [swap(own, "dp", parts, k) for k in order]
    else:
        everyone = [lax.all_gather(own, "dp")]
    tot, wgt, q = totals(own, everyone, steps, parts, c_local, k_local, feats, width)
    q = sum_over(q, "feat")
    centroids, spread = finish(tot, wgt, q, init_centroids, c_local, width)
    return centroids, spread


def solution(mesh):
    in_specs = (P("dp", "feat"), P("dp"), P(None, "dp"), P("dp", "feat"))
    out_specs = (P("dp", "feat"), P(None, "dp"))
    return jax.shard_map(
        per_device, mesh=mesh, in_specs=in_specs, out_specs=out_specs, check_vma=False
    )
```

```python
import functools
import math

import jax
import jax.numpy as jnp
from jax import lax
from jax.experimental import pallas as pl
from jax.experimental.pallas import tpu as pltpu
from jax.sharding import PartitionSpec as P

EPS = 1e-06
LANES = 128
SUBLANES = 8
COUNT_ROW, SQUARE_ROW, LABEL_ROW = 0, 1, 2
SLOT_ROWS = 4
SPLIT = True
HIGHEST = lax.Precision.HIGHEST
F32 = jnp.float32
VMEM = pl.BlockSpec(memory_space=pltpu.VMEM)


def room(*arrays):
    held = sum(4 * math.prod(shape) for shape in arrays)
    return pltpu.CompilerParams(vmem_limit_bytes=min((8 << 20) + 2 * held, 60 << 20))


def swap(x, axis, size, k):
    return lax.ppermute(x, axis, [(i, i ^ k) for i in range(size)])


def sum_over(x, axis):
    size = lax.axis_size(axis)
    if size & (size - 1) or size > 4:
        return lax.psum(x, axis)
    parts = [swap(x, axis, size, k) for k in range(1, size)]
    return functools.reduce(jnp.add, parts, x)


def lanes_of(columns, small=False):
    kind = jnp.bfloat16 if small else F32
    return lax.dot_general(
        jnp.ones((SUBLANES, columns.shape[1]), kind),
        columns.astype(kind),
        (((1,), (1,)), ((), ())),
        precision=None if small else HIGHEST,
        preferred_element_type=F32,
    )


def column_of(row, n):
    r = lax.broadcasted_iota(jnp.int32, (n, row.shape[1]), 0)
    c = lax.broadcasted_iota(jnp.int32, (n, row.shape[1]), 1)
    return jnp.sum(jnp.where(r == c, row, 0.0), axis=1, keepdims=True)


def row_of(column):
    n = column.shape[0]
    r = lax.broadcasted_iota(jnp.int32, (n, LANES), 0)
    c = lax.broadcasted_iota(jnp.int32, (n, LANES), 1)
    return jnp.sum(jnp.where(r == c, column, 0.0), axis=0, keepdims=True)


def sums_kernel(chunks, c_local, groups_of, relative, owner_hbm, assign_hbm, emb_hbm, *rest):
    outs, (owner, assign, emb, acc, cnt, sems) = rest[:-6], rest[-6:]
    n, feats = emb.shape
    cands = acc.shape[0]
    steps = len(chunks)
    starts = [sum(chunks[:s]) for s in range(steps)]

    def copy(s):
        rows = pl.ds(starts[s], chunks[s])
        return pltpu.make_async_copy(emb_hbm.at[rows], emb.at[rows], sems.at[s])

    owners = pltpu.make_async_copy(owner_hbm, owner, sems.at[steps])
    labels = pltpu.make_async_copy(assign_hbm, assign, sems.at[steps + 1])
    owners.start()
    for s in range(steps):
        copy(s).start()
    labels.start()
    owners.wait()
    for s, (start, chunk) in enumerate(zip(starts, chunks)):
        row = lax.broadcasted_iota(jnp.int32, (cands, chunk), 0)
        hit = jnp.where(row == owner[:, start : start + chunk], 1.0, 0.0)
        fold = hit[:, :LANES]
        for j in range(1, chunk // LANES):
            fold = fold + hit[:, j * LANES : (j + 1) * LANES]
        copy(s).wait()
        part = jnp.dot(
            hit.astype(jnp.bfloat16),
            emb[start : start + chunk, :],
            preferred_element_type=F32,
        )
        if s == 0:
            acc[...] = part
            cnt[...] = fold
        else:
            acc[...] += part
            cnt[...] += fold
    labels.wait()
    me = lax.axis_index("dp")
    sub = c_local // SUBLANES
    counts = lanes_of(cnt[...], n <= 256 * LANES)
    if cands % LANES:
        blank = jnp.zeros((SUBLANES, LANES - cands % LANES), F32)
        counts = jnp.concatenate([counts, blank], axis=1)
    tiles = sub * (feats // LANES)
    for out, members in zip(outs, groups_of):
        for slot, k in enumerate(members):
            peer = me ^ k if relative else k
            base = peer * c_local
            dst, at = (out, slot) if relative else (out.at[slot], 0)
            for q in range(feats // LANES):
                for r in range(sub):
                    dst[at * tiles + q * sub + r] = acc[
                        pl.ds(pl.multiple_of(base + r * SUBLANES, SUBLANES), SUBLANES),
                        q * LANES : (q + 1) * LANES,
                    ]
            if at == 0:
                dst[dst.shape[0] - 1] = jnp.zeros((SUBLANES, LANES), F32)
            mine = pltpu.roll(counts, lax.rem(counts.shape[1] - base, counts.shape[1]), 1)
            row = at * SLOT_ROWS + COUNT_ROW
            dst[dst.shape[0] - 1, row : row + 1, :c_local] = mine[:1, :c_local]
            if k == 0 or not relative:
                own = assign[...].astype(F32)
                if not relative:
                    own = jnp.where(me == k, own, 0.0)
                dst[dst.shape[0] - 1, LABEL_ROW : LABEL_ROW + own.shape[0], :c_local] = own


def chunks_of(n):
    quarter = n // 4
    if quarter % (4 * LANES):
        return [LANES] * (n // LANES)
    return [quarter] * 3 + [quarter // 2, quarter // 4, quarter // 4]


def partial_sums(embeddings, owner, assign, parts, groups_of, relative):
    n, feats = embeddings.shape
    c_local = assign.shape[1]
    chunks = chunks_of(n)
    tiles = (c_local // SUBLANES) * (feats // LANES)
    shapes = [
        (len(members) * tiles + 1,) if relative else (len(members), tiles + 1)
        for members in groups_of
    ]
    operands = (owner.reshape(1, n), assign, embeddings)
    return pl.pallas_call(
        functools.partial(sums_kernel, chunks, c_local, groups_of, relative),
        out_shape=[jax.ShapeDtypeStruct((*shape, SUBLANES, LANES), F32) for shape in shapes],
        in_specs=[pl.BlockSpec(memory_space=pltpu.HBM)] * 3,
        out_specs=[VMEM] * len(groups_of),
        scratch_shapes=[
            pltpu.VMEM((1, n), jnp.int32),
            pltpu.VMEM(assign.shape, jnp.int32),
            pltpu.VMEM((n, feats), embeddings.dtype),
            pltpu.VMEM((parts * c_local, feats), F32),
            pltpu.VMEM((parts * c_local, LANES), F32),
            pltpu.SemaphoreType.DMA((len(chunks) + 2,)),
        ],
        compiler_params=pltpu.CompilerParams(vmem_limit_bytes=52 << 20),
        name="candidate_sums",
    )(*[pltpu.with_memory_space_constraint(x, pltpu.HBM) for x in operands])


def other_slot(tile):
    return jnp.concatenate([tile[SLOT_ROWS:], tile[:SLOT_ROWS]], axis=0)


def square_kernel(c_local, slots, *refs):
    ins, out_ref, sq_ref = refs[:-2], refs[-2], refs[-1]
    last = out_ref.shape[0] - 1
    tiles = last // slots
    sub = c_local // SUBLANES
    sq_ref[...] = jnp.zeros_like(sq_ref)
    for slot in range(slots):
        squares = []
        for r in range(sub):
            total = None
            for q in range(tiles // sub):
                t = q * sub + r
                x = ins[0][slot * tiles + t]
                if len(ins) > 1:
                    x = x + ins[1][(slots - 1 - slot) * tiles + t]
                out_ref[slot * tiles + t] = x
                total = x * x if total is None else total + x * x
            squares.append(total)
        lanes = lanes_of(jnp.concatenate(squares, axis=0))
        row = slot * SLOT_ROWS + SQUARE_ROW
        sq_ref[row : row + 1, :c_local] = lanes[:1]
    aux = ins[0][last]
    out_ref[last] = aux + other_slot(ins[1][last]) if len(ins) > 1 else aux


def add_and_square(blocks, c_local, slots):
    shape = blocks[0].shape
    return pl.pallas_call(
        functools.partial(square_kernel, c_local, slots),
        out_shape=[
            jax.ShapeDtypeStruct(shape, F32),
            jax.ShapeDtypeStruct(shape[1:], F32),
        ],
        in_specs=[VMEM] * len(blocks),
        out_specs=[VMEM] * 2,
        compiler_params=room(*[block.shape for block in blocks]),
        name="add_and_square",
    )(*blocks)


def pick(ins, own_ref, raw, c_local, k_local, width, slot, steps):
    cols = raw.shape[1] // LANES
    groups = c_local // SUBLANES
    tiles = groups * cols
    views = []
    for ref in ins:
        if len(ref.shape) == 4:
            views += [(ref.at[j], 0) for j in range(ref.shape[0])]
        else:
            views += [(ref, j) for j in range(ref.shape[0] // tiles)]
    per = LANES // slot
    aux = []
    for n, (view, j) in enumerate(views):
        for r in range(groups):
            at = n * slot + r * SUBLANES
            for q in range(cols):
                raw[at : at + SUBLANES, q * LANES : (q + 1) * LANES] = view[
                    j * tiles + q * groups + r
                ]
        if slot > c_local:
            raw[n * slot + c_local : (n + 1) * slot, :] = jnp.zeros(
                (slot - c_local, cols * LANES), F32
            )
        tile = view[view.shape[0] - 1]
        if j:
            tile = other_slot(tile)
        if n % per == 0:
            aux.append(tile)
        else:
            aux[-1] = aux[-1] + pltpu.roll(tile, slot * (n % per), 1)
    aux = jnp.concatenate(aux, axis=1)
    used = len(views) * slot
    if raw.shape[0] > used:
        raw[used:, :] = jnp.zeros((raw.shape[0] - used, cols * LANES), F32)
    count = aux[COUNT_ROW : COUNT_ROW + 1]
    scale = lax.rsqrt(aux[SQUARE_ROW : SQUARE_ROW + 1] / width + EPS)
    own_aux = own_ref[own_ref.shape[0] - 1]
    first = lax.axis_index("dp") * k_local
    ids = (lax.broadcasted_iota(jnp.int32, (k_local, 1), 0) + first).astype(F32)
    picks, weights = [], []
    for t in range(steps):
        label = LABEL_ROW + t
        own = column_of(own_aux[label : label + 1], c_local)
        keys = jnp.concatenate([ids, own], axis=0)
        match = keys == aux[label : label + 1]
        picks.append(jnp.where(match, count * scale, 0.0))
        weights.append(jnp.sum(jnp.where(match, count, 0.0), axis=1, keepdims=True))
    total = jnp.dot(
        jnp.concatenate(picks, axis=0), raw[...], precision=HIGHEST, preferred_element_type=F32
    )
    return total, jnp.concatenate(weights, axis=0)


def early_kernel(sizes, own_ref, *refs):
    ins, (tot_ref, wgt_ref, raw) = refs[:-3], refs[-3:]
    total, weight = pick(ins, own_ref, raw, *sizes)
    tot_ref[...] = total
    wgt_ref[...] = jnp.broadcast_to(weight, wgt_ref.shape)


def totals_kernel(sizes, n_in, own_ref, init_ref, *refs):
    c_local, k_local, width, _, steps = sizes
    ins, prior, (base_ref, wgt_ref, q_ref, raw) = refs[:n_in], refs[n_in:-4], refs[-4:]
    total, weights = pick(ins, own_ref, raw, *sizes)
    if prior:
        total = total + prior[0][...]
        weights = weights + prior[1][:, :1]
    cols = raw.shape[1] // LANES
    groups = c_local // SUBLANES
    own_square = own_ref[own_ref.shape[0] - 1][SQUARE_ROW : SQUARE_ROW + 1]
    means = jnp.concatenate(
        [
            jnp.concatenate([own_ref[q * groups + r] for q in range(cols)], axis=1)
            for r in range(groups)
        ],
        axis=0,
    ) * lax.rsqrt(column_of(own_square, c_local) / width + EPS)
    span = k_local + c_local
    lane = lax.broadcasted_iota(jnp.int32, (c_local, LANES), 1)
    q_c = jnp.zeros((c_local, LANES), F32)
    w_c = jnp.zeros((c_local, LANES), F32)
    base = init_ref[...]
    length = jnp.zeros((k_local, 1), F32)
    fresh = jnp.zeros((k_local, 1), F32)
    for t in range(steps):
        t_k = total[t * span : t * span + k_local]
        t_c = total[t * span + k_local : (t + 1) * span]
        weight = weights[t * span : t * span + k_local]
        near = weights[t * span + k_local : (t + 1) * span]
        center = t_c / jnp.where(near > 0, near, 1.0)
        diff = means - center
        for j, (a, b) in enumerate(((diff, diff), (diff, center), (center, center))):
            q_c = jnp.where(lane == 4 * t + j, jnp.sum(a * b, axis=1, keepdims=True), q_c)
        w_c = jnp.where(lane == t, near, w_c)
        base = jnp.where(weight > 0, t_k, base)
        length = jnp.where(weight > 0, jnp.sum(t_k * t_k, axis=1, keepdims=True), length)
        fresh = jnp.where(weight > 0, 1.0, fresh)
    base_ref[...] = base
    q_ref[:c_local] = q_c
    q_ref[c_local:] = jnp.broadcast_to(length, (k_local, LANES))
    wgt_ref[:c_local] = w_c
    wgt_ref[c_local:] = jnp.broadcast_to(fresh, (k_local, LANES))


def totals(own, early, late, init, steps, c_local, width):
    k_local, feats = init.shape
    slot = 8
    while slot < c_local:
        slot *= 2
    tiles = (c_local // SUBLANES) * (feats // LANES)

    def lanes(arrays):
        blocks = sum(x.shape[0] if len(x.shape) == 4 else x.shape[0] // tiles for x in arrays)
        return -(-blocks * slot // LANES) * LANES

    sizes = (c_local, k_local, width, slot, steps)
    rows = c_local + k_local
    prior = ()
    if early:
        prior = pl.pallas_call(
            functools.partial(early_kernel, sizes),
            out_shape=[
                jax.ShapeDtypeStruct((steps * rows, feats), F32),
                jax.ShapeDtypeStruct((steps * rows, LANES), F32),
            ],
            in_specs=[VMEM] * (1 + len(early)),
            out_specs=[VMEM] * 2,
            scratch_shapes=[pltpu.VMEM((lanes(early), feats), F32)],
            compiler_params=room((lanes(early), 2 * feats)),
            name="early_totals",
        )(own, *early)
    return pl.pallas_call(
        functools.partial(totals_kernel, sizes, len(late)),
        out_shape=[
            jax.ShapeDtypeStruct((k_local, feats), F32),
            jax.ShapeDtypeStruct((rows, LANES), F32),
            jax.ShapeDtypeStruct((rows, LANES), F32),
        ],
        in_specs=[VMEM] * (2 + len(late) + len(prior)),
        out_specs=[VMEM] * 3,
        scratch_shapes=[pltpu.VMEM((lanes(late), feats), F32)],
        compiler_params=room((lanes(late), 2 * feats)),
        name="cluster_totals",
    )(own, init, *late, *prior)


def finish_kernel(steps, width, base_ref, wgt_ref, q_ref, cen_hbm, spread_hbm, cen, spread, sems):
    k_local = cen.shape[0]
    c_local = wgt_ref.shape[0] - k_local
    length = q_ref[c_local:, :1]
    scale = jnp.where(wgt_ref[c_local:, :1] > 0, lax.rsqrt(length / width + EPS), 1.0)
    cen[...] = base_ref[...] * scale
    first = pltpu.make_async_copy(cen, cen_hbm, sems.at[0])
    first.start()
    for t in range(steps):
        near = wgt_ref[:c_local, t : t + 1]
        dd, da, aa = (q_ref[:c_local, 4 * t + j : 4 * t + j + 1] for j in range(3))
        gap = 1.0 - near * lax.rsqrt(near * near * (aa / width) + EPS)
        spread[t : t + 1, :] = row_of((dd + gap * (2.0 * da + gap * aa)) / width)[:, :c_local]
    second = pltpu.make_async_copy(spread, spread_hbm, sems.at[1])
    second.start()
    first.wait()
    second.wait()


def finish(base, wgt, q, steps, width):
    c_local = wgt.shape[0] - base.shape[0]
    shapes = (base.shape, (steps, c_local))
    return pl.pallas_call(
        functools.partial(finish_kernel, steps, width),
        out_shape=[jax.ShapeDtypeStruct(shape, F32) for shape in shapes],
        in_specs=[VMEM] * 3,
        out_specs=[pl.BlockSpec(memory_space=pltpu.HBM)] * 2,
        scratch_shapes=[pltpu.VMEM(shape, F32) for shape in shapes]
        + [pltpu.SemaphoreType.DMA((2,))],
        compiler_params=room(base.shape),
        name="finish",
    )(base, wgt, q)


def per_device(embeddings, sample_owner, lloyd_assign, init_centroids):
    parts = lax.axis_size("dp")
    steps, c_local = lloyd_assign.shape
    k_local, feats = init_centroids.shape
    width = feats * lax.axis_size("feat")
    top = parts // 2
    direct = 2 <= parts <= 16 and parts & (parts - 1) == 0
    order = sorted(range(1, top), key=lambda k: (k.bit_count(), -k))
    if direct:
        groups_of = [(k, k ^ top) for k in range(top)]
    else:
        groups_of = [tuple(range(parts))]
    blocks = partial_sums(embeddings, sample_owner, lloyd_assign, parts, groups_of, direct)
    if direct:
        near = [swap(blocks[k], "dp", parts, k) for k in order]
        pair = functools.reduce(jnp.add, near, blocks[0])
        blocks = [pair, swap(pair, "dp", parts, top)]
    else:
        blocks = [lax.psum_scatter(blocks[0], "dp", scatter_dimension=0)]
    own, squares = add_and_square(blocks, c_local, 2 if direct else 1)
    own = own.at[-1].add(sum_over(squares, "feat"))
    if direct:
        got = {k: swap(own, "dp", parts, k) for k in order}
        early = [own] + [got[k] for k in order[2:]] if SPLIT else []
        late = [got[k] for k in order[:2]] if SPLIT else [own] + list(got.values())
    else:
        early, late = [], [lax.all_gather(own, "dp")]
    base, wgt, q = totals(own, early, late, init_centroids, steps, c_local, width)
    return tuple(finish(base, wgt, sum_over(q, "feat"), steps, width))


def solution(mesh):
    in_specs = (P("dp", "feat"), P("dp"), P(None, "dp"), P("dp", "feat"))
    out_specs = (P("dp", "feat"), P(None, "dp"))
    return jax.shard_map(
        per_device, mesh=mesh, in_specs=in_specs, out_specs=out_specs, check_vma=False
    )
```
